32 devices in a mesh: group: 2 (over x), area: 16 (over z, y, core).
Axes of the slice: x: 2, y: 2, z: 4, core: 2. Of those that a mesh axis runs over, the one named last changes fastest.
Arguments:
- state_init: float32 [64, 12288], P('group', 'area'), parts along dimension 0, may hold values from -6 to 6
- prior_interval_trace: bfloat16 [4, 64, 12288], P(None, 'group', 'area'), parts along dimension 1, may hold values from -0.8984375 to 0.8984375
- drive_input: bfloat16 [64, 12288], P('group', 'area'), parts along dimension 0, may hold values from -4 to 4
- leak_rate: float32 [24576], P(('group', 'area')), parts along dimension 0, may hold values from 0.15 to 1
- w_recur: bfloat16 [24576, 6144], P(('group', 'area')), parts along dimension 0, may hold values from -0.078125 to 0.078125
- w_send: bfloat16 [24576, 768], P(('group', 'area')), parts along dimension 0, may hold values from -0.078125 to 0.078125
- w_recv: bfloat16 [24576, 768], P(('group', 'area')), parts along dimension 0, may hold values from -0.21875 to 0.21875
- area_mask: int32 [4, 2], P('group'), parts along dimension 0, may hold values 0 or 1
- coupling: float32 [4, 2], P('group'), parts along dimension 0, may hold values from 0.1 to 0.6
- delay_slot: int32 [4, 2], P('group'), parts along dimension 0, may hold values from 0 to 3
Outputs:
- final_state: float32 [64, 12288], P('group', 'area'), parts along dimension 0
- final_history: bfloat16 [4, 64, 12288], P(None, 'group', 'area'), parts along dimension 1
The draws below stay inside these ranges and needn't reach their ends.
There are 2 independent parts, one for each index of `group`. The reference program is written for one: setup_inputs(seed, part) draws one part's arguments, and reference() takes and returns one part's arrays. A program takes and returns all parts, laid end to end along the dimension named above; each array names one. Nothing has to cross between parts.
All inputs are finite; a program needn't handle non-finite values.
Results may differ from the reference program's by a relative error of at most 0.0095.
Values may be sent and summed in bfloat16 or wider, within the bound.
A program may use at most 64 MiB of HBM per device.

```python
import math
import jax
import jax.numpy as jnp
from jax import lax

NEURONS_REGION = 6144
RANK = 768
LAG_TICKS = 4
INTERVALS = 2
EPISODE_TALLY = 32
REGION_TALLY = 2
ALL_UNITS = 12288


def set_ends(drawn, stream_key, smallest, high):
    longest = drawn.shape.index(max(drawn.shape))
    spots = []
    for shift in (0, 1):
        where = [jax.random.randint(jax.random.fold_in(stream_key, axis), (), 0, length) for axis, length in enumerate(drawn.shape)]
        where[longest] = (where[longest] + shift) % drawn.shape[longest]
        spots.append(tuple(where))
    return drawn.at[spots[0]].set(smallest).at[spots[1]].set(high)


def shard_levels(own_key, shape, shards, least, top_value):
    gain = 1.0
    for axis_at, shards_of in shards:
        heights = jax.random.uniform(jax.random.fold_in(jax.random.fold_in(own_key, 6), axis_at), (shards_of,), jnp.float32, least / len(shards), top_value / len(shards))
        gain = gain * jnp.repeat(jnp.exp(heights), shape[axis_at] // shards_of).reshape((-1,) + (1,) * (len(shape) - 1 - axis_at))
    return gain


def noise(stream_key, shape, deviation, limit, split=(), kind=jnp.bfloat16):
    values = jax.random.normal(stream_key, shape, jnp.float32) * deviation
    if len(split) > 0:
        values = shard_levels(stream_key, shape, split, -0.22, 0.18) * values
    return jnp.clip(values, min=-limit, max=limit).astype(kind)


def setup_inputs(seed: int = 0, part: int = 0) -> dict:
    streams_of = jax.random.split(jax.random.key(seed), 11)
    own_keys = jax.random.split(jax.random.fold_in(streams_of[10], part), 11)
    state_init = noise(own_keys[0], (EPISODE_TALLY, ALL_UNITS), 1.0, 6.0, ((1, 16),), jnp.float32)
    prior_interval_trace = jnp.clip(jax.random.uniform(own_keys[1], (LAG_TICKS, EPISODE_TALLY, ALL_UNITS), jnp.float32, -0.8984375, 0.8984375) * shard_levels(own_keys[1], (LAG_TICKS, EPISODE_TALLY, ALL_UNITS), ((2, 16),), -0.4, 0.0), -0.8984375, 0.8984375).astype(jnp.bfloat16)
    drive_input = noise(own_keys[2], (EPISODE_TALLY, ALL_UNITS), 0.5, 4.0, ((1, 16),))
    leak_rate = jnp.clip(jnp.exp(math.log(1.0) - 1.89712 * jax.random.uniform(own_keys[3], (ALL_UNITS,), jnp.float32) ** shard_levels(own_keys[3], (ALL_UNITS,), ((0, 16),), -0.2, 0.2)), 0.15, 1.0)
    w_recur = noise(own_keys[4], (ALL_UNITS, NEURONS_REGION), NEURONS_REGION ** -0.5, 0.078125, ((0, 16),))
    w_send = noise(own_keys[5], (ALL_UNITS, RANK), NEURONS_REGION ** -0.5, 0.078125, ((0, 16),))
    w_recv = noise(own_keys[6], (ALL_UNITS, RANK), RANK ** -0.5, 0.21875, ((0, 16),))
    area_mask = set_ends((jax.random.randint(own_keys[7], (REGION_TALLY, REGION_TALLY), 0, 2) < 1).astype(jnp.int32), jax.random.fold_in(own_keys[7], 1), 0, 1)
    coupling = jnp.clip(jnp.exp(jax.random.uniform(own_keys[8], (REGION_TALLY, REGION_TALLY), jnp.float32, math.log(0.1), math.log(0.6))), 0.1, 0.6)
    delay_slot = set_ends(jax.random.randint(own_keys[9], (REGION_TALLY, REGION_TALLY), 0, LAG_TICKS), jax.random.fold_in(own_keys[9], 1), 0, LAG_TICKS - 1).astype(jnp.int32)
    return dict(state_init=state_init, prior_interval_trace=prior_interval_trace, drive_input=drive_input, leak_rate=leak_rate, w_recur=w_recur, w_send=w_send, w_recv=w_recv, area_mask=area_mask, coupling=coupling, delay_slot=delay_slot)


def reference(state_init, prior_interval_trace, drive_input, leak_rate, w_recur, w_send, w_recv, area_mask, coupling, delay_slot):
    strength = area_mask.astype(jnp.float32) * coupling
    slots = jnp.arange(LAG_TICKS, dtype=jnp.int32)
    selector = (delay_slot[:, :, None] == slots[None, None, :]).astype(jnp.float32) * strength[:, :, None]
    recur_blocks = w_recur.reshape(REGION_TALLY, NEURONS_REGION, NEURONS_REGION)
    send_blocks = w_send.astype(jnp.float32).reshape(REGION_TALLY, NEURONS_REGION, RANK)
    recv_blocks = w_recv.astype(jnp.float32).reshape(REGION_TALLY, NEURONS_REGION, RANK)

    def remote_input(history):
        spread = history.astype(jnp.float32).reshape(LAG_TICKS, EPISODE_TALLY, REGION_TALLY, NEURONS_REGION)
        readout = jnp.einsum("ktbs,bsr->ktbr", spread, send_blocks, precision=lax.Precision.HIGHEST)
        summed = jnp.einsum("abk,ktbr->atr", selector, readout, precision=lax.Precision.HIGHEST)
        summed = summed.astype(jnp.bfloat16).astype(jnp.float32)
        result = jnp.einsum("atr,aur->tau", summed, recv_blocks, precision=lax.Precision.HIGHEST)
        return result.reshape(EPISODE_TALLY, REGION_TALLY * NEURONS_REGION)

    def one_area(pair):
        rates_area, weights_area = pair
        return jnp.dot(rates_area, weights_area.T, preferred_element_type=jnp.float32)

    def lateral_feedback(spiking_activity):
        sorted_per_region = jnp.transpose(spiking_activity.reshape(EPISODE_TALLY, REGION_TALLY, NEURONS_REGION), (1, 0, 2))
        result = lax.map(one_area, (sorted_per_region, recur_blocks))
        return jnp.transpose(result, (1, 0, 2)).reshape(EPISODE_TALLY, REGION_TALLY * NEURONS_REGION)

    drive = drive_input.astype(jnp.float32)
    neuron_voltage = state_init
    history = prior_interval_trace
    spiking_activity = prior_interval_trace[LAG_TICKS - 1]
    for interval in range(INTERVALS):
        remote = remote_input(history)
        logged_activity = []
        for step_index in range(LAG_TICKS):
            lateral_forcing = lateral_feedback(spiking_activity)
            neuron_voltage = neuron_voltage + leak_rate[None, :] * (-neuron_voltage + lateral_forcing + remote + drive)
            spiking_activity = jnp.tanh(neuron_voltage).astype(jnp.bfloat16)
            logged_activity.append(spiking_activity)
        history = jnp.stack(logged_activity)
    return neuron_voltage, history
```

```python
import functools

import jax
import jax.numpy as jnp
from jax import lax
from jax.experimental import pallas as pl
from jax.experimental.pallas import tpu as pltpu
from jax.sharding import PartitionSpec as P

INTERVALS = 2
TRANSPOSED = (((1,), (1,)), ((), ()))


def flip(index, mask):
    bit = 1
    while bit <= mask:
        if mask & bit:
            index = index + bit - 2 * bit * ((index // bit) % 2)
        bit *= 2
    return index


def kernel(
    devices, split, state, prior, drive, leak, w_recur, w_send, w_recv, mask, coupling, delay,
    voltage, history,
    w_rec, w_snd, w_rcv, rates, readout, outgoing, incoming, subspace, base,
    w_sem, send_sem, fwd_sem, recv_sem, out_sem, in_sem, sub_send, sub_recv,
):
    me = lax.axis_index("area")
    place = me % split
    area = me // split
    areas = devices // split
    ticks, trials, units = prior.shape
    rows = trials // split
    forwarded = range(2, split, 2)

    def load_recur(m):
        start = pl.multiple_of(flip(place, m) * units, units)
        return pltpu.make_async_copy(w_recur.at[:, pl.ds(start, units)], w_rec.at[m], w_sem.at[m])

    load_send = pltpu.make_async_copy(w_send, w_snd, w_sem.at[split])
    load_recv = pltpu.make_async_copy(w_recv, w_rcv, w_sem.at[split + 1])

    load_send.start()
    for m in range(split):
        load_recur(m).start()
    load_recv.start()

    barrier = pltpu.get_barrier_semaphore()

    @pl.loop(1, devices)
    def _(o):
        pl.semaphore_signal(barrier, inc=1, device_id={"area": (me + o) % devices})

    voltage[...] = state[...]
    rates[0, 0] = prior[ticks - 1]
    load_send.wait()
    for k in range(ticks - 1):
        readout[k] = jnp.dot(prior[k], w_snd[...], preferred_element_type=jnp.float32)
    pl.semaphore_wait(barrier, devices - 1)

    def rate_copy(par, m):
        return pltpu.make_async_remote_copy(
            src_ref=rates.at[par, 0], dst_ref=rates.at[par, m],
            send_sem=send_sem.at[m], recv_sem=recv_sem.at[par, m],
            device_id={"area": flip(me, m)},
        )

    def rate_forward(par, m):
        return pltpu.make_async_remote_copy(
            src_ref=rates.at[par, m], dst_ref=rates.at[par, m + 1],
            send_sem=fwd_sem.at[m], recv_sem=recv_sem.at[par, m + 1],
            device_id={"area": flip(me, 1)},
        )

    def part_copy(it, o):
        target = (me + o) % devices
        return pltpu.make_async_remote_copy(
            src_ref=outgoing.at[target // split, target % split], dst_ref=incoming.at[it, o],
            send_sem=out_sem.at[o], recv_sem=in_sem.at[it, o],
            device_id={"area": target},
        )

    def sub_copy(it, m):
        return pltpu.make_async_remote_copy(
            src_ref=subspace.at[it, place], dst_ref=subspace.at[it, place],
            send_sem=sub_send.at[m], recv_sem=sub_recv.at[it, m],
            device_id={"area": flip(me, m)},
        )

    def matmul(par, m):
        return lax.dot_general(rates[par, m], w_rec[m], TRANSPOSED, preferred_element_type=jnp.float32)

    def step(it, k, first):
        par = (it * ticks + k) % 2

        def ready(m):
            if first:
                @pl.when(it == 0)
                def _():
                    load_recur(m).wait()

        for m in reversed(forwarded):
            rate_copy(par, m).start()
        rate_copy(par, 1).start()
        readout[(k + ticks - 1) % ticks] = jnp.dot(
            rates[par, 0], w_snd[...], preferred_element_type=jnp.float32
        )
        if first:
            for a in range(areas):
                strength = mask[a, area].astype(jnp.float32) * coupling[a, area]
                part = readout[delay[a, area]] * strength
                for j in range(split):
                    outgoing[a, j] = part[j * rows : (j + 1) * rows]

            @pl.loop(1, devices)
            def _(o):
                part_copy(it, o).start()

        ready(0)
        acc = matmul(par, 0)
        if not first:
            acc = acc + base[...]
        rate_copy(par, 1).wait_recv()
        ready(1)
        acc = acc + matmul(par, 1)
        *early, late = forwarded
        for m in early:
            rate_copy(par, m).wait_recv()
            rate_forward(par, m).start()
        for m in early:
            ready(m)
            acc = acc + matmul(par, m)
        rate_copy(par, late).wait_recv()
        rate_forward(par, late).start()
        if first:
            def add(o, total):
                part_copy(it, o).wait_recv()
                return total + incoming[it, o]

            subspace[it, place] = lax.fori_loop(1, devices, add, outgoing[area, place])
            for m in range(1, split):
                sub_copy(it, m).start()
        for m in early:
            rate_forward(par, m).wait_recv()
            ready(m + 1)
            acc = acc + matmul(par, m + 1)
        ready(late)
        acc = acc + matmul(par, late)
        rate_forward(par, late).wait_recv()
        ready(late + 1)
        acc = acc + matmul(par, late + 1)
        if first:
            for m in range(1, split):
                sub_copy(it, m).wait_recv()

            @pl.when(it == 0)
            def _():
                load_recv.wait()

            summed = jnp.concatenate([subspace[it, j] for j in range(split)], 0).astype(jnp.bfloat16)
            base[...] = drive[...].astype(jnp.float32) + lax.dot_general(
                summed, w_rcv[...], TRANSPOSED, preferred_element_type=jnp.float32
            )
            acc = acc + base[...]
            for m in range(1, split):
                sub_copy(it, m).wait_send()

            @pl.loop(1, devices)
            def _(o):
                part_copy(it, o).wait_send()

        rate_copy(par, 1).wait_send()
        for m in forwarded:
            rate_copy(par, m).wait_send()
            rate_forward(par, m).wait_send()
        potential = voltage[...]
        potential = potential + leak[...] * (acc - potential)
        voltage[...] = potential
        firing = jnp.tanh(potential).astype(jnp.bfloat16)
        history[k] = firing
        rates[1 - par, 0] = firing

    @pl.loop(0, INTERVALS)
    def _(it):
        step(it, 0, True)

        @pl.loop(1, ticks)
        def _(k):
            step(it, k, False)


def body(
    devices, state_init, prior_interval_trace, drive_input, leak_rate, w_recur, w_send, w_recv,
    area_mask, coupling, delay_slot,
):
    ticks, trials, units = prior_interval_trace.shape
    rank = w_send.shape[1]
    split = w_recur.shape[1] // units
    areas = devices // split
    rows = trials // split
    vmem = pl.BlockSpec(memory_space=pltpu.VMEM)
    smem = pl.BlockSpec(memory_space=pltpu.SMEM)
    hbm = pl.BlockSpec(memory_space=pl.ANY)
    dma = pltpu.SemaphoreType.DMA
    return pl.pallas_call(
        functools.partial(kernel, devices, split),
        out_shape=(
            jax.ShapeDtypeStruct(state_init.shape, jnp.float32),
            jax.ShapeDtypeStruct(prior_interval_trace.shape, jnp.bfloat16),
        ),
        in_specs=[vmem, vmem, vmem, vmem, hbm, hbm, hbm, smem, smem, smem],
        out_specs=(vmem, vmem),
        scratch_shapes=[
            pltpu.VMEM((split, units, units), jnp.bfloat16),
            pltpu.VMEM((units, rank), jnp.bfloat16),
            pltpu.VMEM((units, rank), jnp.bfloat16),
            pltpu.VMEM((2, split, trials, units), jnp.bfloat16),
            pltpu.VMEM((ticks, trials, rank), jnp.float32),
            pltpu.VMEM((areas, split, rows, rank), jnp.float32),
            pltpu.VMEM((INTERVALS, devices, rows, rank), jnp.float32),
            pltpu.VMEM((INTERVALS, split, rows, rank), jnp.float32),
            pltpu.VMEM((trials, units), jnp.float32),
            dma((split + 2,)),
            dma((split,)),
            dma((split,)),
            dma((2, split)),
            dma((devices,)),
            dma((INTERVALS, devices)),
            dma((split,)),
            dma((INTERVALS, split)),
        ],
        compiler_params=pltpu.CompilerParams(
            collective_id=0, has_side_effects=True, vmem_limit_bytes=48 * 1024 * 1024
        ),
    )(
        state_init, prior_interval_trace, drive_input, leak_rate.reshape(1, units),
        w_recur, w_send, w_recv, area_mask, coupling, delay_slot,
    )


def solution(mesh):
    in_specs = (
        P("group", "area"),
        P(None, "group", "area"),
        P("group", "area"),
        P(("group", "area")),
        P(("group", "area"), None),
        P(("group", "area"), None),
        P(("group", "area"), None),
        P("group", None),
        P("group", None),
        P("group", None),
    )
    out_specs = (P("group", "area"), P(None, "group", "area"))
    return jax.shard_map(
        functools.partial(body, mesh.shape["area"]),
        mesh=mesh, in_specs=in_specs, out_specs=out_specs, check_vma=False,
    )
```
